32 devices in a mesh: fsdp: 4 (over z), ctx: 4 (over y, x), tp: 2 (over core).
Axes of the slice: x: 2, y: 2, z: 4, core: 2. Of those that a mesh axis runs over, the one named last changes fastest.
Arguments:
- frames: bfloat16 [8, 1024, 1024], P('fsdp', 'ctx'), may hold values from -6 to 6
- sequence_adapter: int32 [8], replicated, may hold values from 0 to 7
- feedforward_up_weight: bfloat16 [1, 2, 1024, 4096], P(None, None, 'fsdp', 'tp'), may hold values from -0.1875 to 0.1875
- feedforward_down_weight: bfloat16 [1, 2, 4096, 1024], P(None, None, 'tp', 'fsdp'), may hold values from -0.09375 to 0.09375
- query_key_value_weight: bfloat16 [1, 1024, 3, 1024], P(None, 'fsdp', None, 'tp'), may hold values from -0.1875 to 0.1875
- attention_output_weight: bfloat16 [1, 1024, 1024], P(None, 'tp', 'fsdp'), may hold values from -2 to 2
- pointwise_first_weight: bfloat16 [1, 1024, 2, 1024], P(None, 'fsdp', None, 'tp'), may hold values from -0.1875 to 0.1875
- depthwise_weight: float32 [1, 9, 1024], P(None, None, 'tp'), may hold values from -2 to 2
- batchnorm_scale: float32 [1, 1024], P(None, 'tp'), may hold values from 0.5 to 1.5
- batchnorm_bias: float32 [1, 1024], P(None, 'tp'), may hold values from -3 to 3
- pointwise_second_weight: bfloat16 [1, 1024, 1024], P(None, 'tp', 'fsdp'), may hold values from -0.1875 to 0.1875
- layernorm_scale: float32 [1, 5, 1024], replicated, may hold values from 0.5 to 1.5
- layernorm_bias: float32 [1, 5, 1024], replicated, may hold values from -1.75 to 1.75
- adapter_reader_down: bfloat16 [1, 6, 8, 1024, 16], replicated, may hold values from -0.1875 to 0.1875
- adapter_first_up: bfloat16 [1, 2, 8, 16, 4096], replicated, may hold values from -0.75 to 0.75
- adapter_query_key_up: bfloat16 [1, 3, 8, 16, 1024], replicated, may hold values from -0.75 to 0.75
- adapter_gating_up: bfloat16 [1, 8, 16, 2, 1024], replicated, may hold values from -0.75 to 0.75
- adapter_second_down: bfloat16 [1, 2, 8, 4096, 16], replicated, may hold values from -0.09375 to 0.09375
- adapter_mixing_down: bfloat16 [1, 2, 8, 1024, 16], replicated, may hold values from -0.1875 to 0.1875
- adapter_writer_up: bfloat16 [1, 4, 8, 16, 1024], replicated, may hold values from -0.75 to 0.75
- final_output_gradient: bfloat16 [8, 1024, 1024], P('fsdp', 'ctx'), may hold values from -6 to 6
Outputs:
- encoded: bfloat16 [8, 1024, 1024], P('fsdp', 'ctx')
- frames_grad: float32 [8, 1024, 1024], P('fsdp', 'ctx')
- grad_in_a: float32 [1, 6, 8, 1024, 16], P(None, None, None, None, 'fsdp')
- grad_up_b: float32 [1, 2, 8, 16, 4096], P(None, None, None, 'fsdp', 'tp')
- grad_qkv_b: float32 [1, 3, 8, 16, 1024], P(None, None, None, 'fsdp', 'tp')
- grad_glu_b: float32 [1, 8, 16, 2, 1024], P(None, None, 'fsdp', None, 'tp')
- grad_down_a: float32 [1, 2, 8, 4096, 16], P(None, None, None, 'tp', 'fsdp')
- grad_mix_a: float32 [1, 2, 8, 1024, 16], P(None, None, None, 'tp', 'fsdp')
- grad_out_b: float32 [1, 4, 8, 16, 1024], P(None, None, None, 'fsdp')
The draws below stay inside these ranges and needn't reach their ends.
All inputs are finite; a program needn't handle non-finite values.
Results may differ from the reference program's by a relative error of at most 0.039.
Values may be sent and summed in bfloat16 or wider, within the bound.
A program may use at most 256 MiB of HBM per device.

```python
import math
import jax
import jax.numpy as jnp
from jax import lax

MODEL_DIM = 1024
HIDDEN_UNITS = 4096
HEADS = 8
KW = 9
ADAPTER_RANK = 16
ADAPTER_NUMBER = 8
ENCODER_DEPTH = 1
LEN = 1024
SEQS = 8


def plant(drawn, own_key, least, high):
    spot = [jax.random.randint(jax.random.fold_in(own_key, axis), (), 0, length) for axis, length in enumerate(drawn.shape)]
    main_axis = drawn.shape.index(max(drawn.shape))
    beside = spot[:main_axis] + [(spot[main_axis] + 1) % drawn.shape[main_axis]] + spot[main_axis + 1:]
    return drawn.at[tuple(spot)].set(least).at[tuple(beside)].set(high)


def levels(rng, shape, cuts, low, largest):
    def one(axis_at, shards_of):
        draws = jax.random.uniform(jax.random.fold_in(jax.random.fold_in(rng, 6), axis_at), (shards_of,), jnp.float32, low / len(cuts), largest / len(cuts))
        return jnp.repeat(jnp.exp(draws), shape[axis_at] // shards_of).reshape((-1,) + (1,) * (len(shape) - axis_at - 1))

    factor_of = one(*cuts[0])
    for cut in cuts[1:]:
        factor_of = factor_of * one(*cut)
    return factor_of


def normal_values(own_key, dims, scale, reach, split=(), kind=jnp.bfloat16):
    entries = jax.random.normal(own_key, dims, jnp.float32) * scale
    if len(split) > 0:
        entries = levels(own_key, dims, split, -0.22, 0.18) * entries
    return jnp.clip(entries, min=-reach, max=reach).astype(kind)


def setup_inputs(seed: int = 0) -> dict:
    arg_keys = jax.random.split(jax.random.key(seed), 22)
    return {
        "frames": normal_values(arg_keys[0], (SEQS, LEN, MODEL_DIM), 1.0, 6.0, ((0, 4), (1, 4))),
        "sequence_adapter": plant(jax.random.randint(arg_keys[1], (SEQS,), 0, ADAPTER_NUMBER), jax.random.fold_in(arg_keys[1], 1), 0, ADAPTER_NUMBER - 1).astype(jnp.int32),
        "feedforward_up_weight": normal_values(arg_keys[2], (ENCODER_DEPTH, 2, MODEL_DIM, HIDDEN_UNITS), MODEL_DIM ** -0.5, 0.1875, ((2, 4), (3, 2))),
        "feedforward_down_weight": normal_values(arg_keys[3], (ENCODER_DEPTH, 2, HIDDEN_UNITS, MODEL_DIM), HIDDEN_UNITS ** -0.5, 0.09375, ((2, 2), (3, 4))),
        "query_key_value_weight": normal_values(arg_keys[4], (ENCODER_DEPTH, MODEL_DIM, 3, MODEL_DIM), MODEL_DIM ** -0.5, 0.1875, ((1, 4), (3, 2))),
        "attention_output_weight": normal_values(arg_keys[5], (ENCODER_DEPTH, MODEL_DIM, MODEL_DIM), (max(MODEL_DIM // 128, 1)) ** -0.5, 2.0, ((1, 2), (2, 4))),
        "pointwise_first_weight": normal_values(arg_keys[6], (ENCODER_DEPTH, MODEL_DIM, 2, MODEL_DIM), MODEL_DIM ** -0.5, 0.1875, ((1, 4), (3, 2))),
        "depthwise_weight": normal_values(arg_keys[7], (ENCODER_DEPTH, KW, MODEL_DIM), KW ** -0.5, 2.0, ((2, 2),), jnp.float32),
        "batchnorm_scale": jnp.clip(1.0 + 0.1 * jax.random.normal(arg_keys[8], (ENCODER_DEPTH, MODEL_DIM), jnp.float32), 0.5, 1.5),
        "batchnorm_bias": normal_values(arg_keys[9], (ENCODER_DEPTH, MODEL_DIM), 0.5, 3.0, ((1, 2),), jnp.float32),
        "pointwise_second_weight": normal_values(arg_keys[10], (ENCODER_DEPTH, MODEL_DIM, MODEL_DIM), MODEL_DIM ** -0.5, 0.1875, ((1, 2), (2, 4))),
        "layernorm_scale": jnp.clip(1.0 + 0.1 * jax.random.normal(arg_keys[11], (ENCODER_DEPTH, 5, MODEL_DIM), jnp.float32), 0.5, 1.5),
        "layernorm_bias": normal_values(arg_keys[12], (ENCODER_DEPTH, 5, MODEL_DIM), 0.3, 1.75, (), jnp.float32),
        "adapter_reader_down": normal_values(arg_keys[13], (ENCODER_DEPTH, 6, ADAPTER_NUMBER, MODEL_DIM, ADAPTER_RANK), MODEL_DIM ** -0.5, 0.1875),
        "adapter_first_up": normal_values(arg_keys[14], (ENCODER_DEPTH, 2, ADAPTER_NUMBER, ADAPTER_RANK, HIDDEN_UNITS), (4 * ADAPTER_RANK) ** -0.5, 0.75),
        "adapter_query_key_up": normal_values(arg_keys[15], (ENCODER_DEPTH, 3, ADAPTER_NUMBER, ADAPTER_RANK, MODEL_DIM), (4 * ADAPTER_RANK) ** -0.5, 0.75),
        "adapter_gating_up": normal_values(arg_keys[16], (ENCODER_DEPTH, ADAPTER_NUMBER, ADAPTER_RANK, 2, MODEL_DIM), (4 * ADAPTER_RANK) ** -0.5, 0.75),
        "adapter_second_down": normal_values(arg_keys[17], (ENCODER_DEPTH, 2, ADAPTER_NUMBER, HIDDEN_UNITS, ADAPTER_RANK), HIDDEN_UNITS ** -0.5, 0.09375),
        "adapter_mixing_down": normal_values(arg_keys[18], (ENCODER_DEPTH, 2, ADAPTER_NUMBER, MODEL_DIM, ADAPTER_RANK), MODEL_DIM ** -0.5, 0.1875),
        "adapter_writer_up": normal_values(arg_keys[19], (ENCODER_DEPTH, 4, ADAPTER_NUMBER, ADAPTER_RANK, MODEL_DIM), (4 * ADAPTER_RANK) ** -0.5, 0.75),
        "final_output_gradient": normal_values(arg_keys[20], (SEQS, LEN, MODEL_DIM), 1.0, 6.0, ((0, 4), (1, 4))),
    }


EPS = 1e-05
HIGHEST = lax.Precision.HIGHEST

@jax.custom_vjp
def low(v):
    return lax.optimization_barrier(v.astype(jnp.bfloat16)).astype(jnp.float32)

@jax.custom_vjp
def low_back(v):
    return v

def low_keep(v):
    return (low(v), None)

def low_pass(kept, grad):
    return (grad,)

def back_keep(v):
    return (v, None)

def back_low(kept, grad):
    return (low(grad),)
low.defvjp(low_keep, low_pass)
low_back.defvjp(back_keep, back_low)

def layer_norm(values, gain_row, shift_row):
    centre = lax.optimization_barrier(jnp.mean(values, axis=-1, keepdims=True))
    centred = values - centre
    spread = lax.optimization_barrier(jnp.mean(centred * centred, axis=-1, keepdims=True))
    return centred * lax.rsqrt(spread + EPS) * gain_row + shift_row

def product(spec, left, right):
    return jnp.einsum(spec, left, right, precision=HIGHEST)

def adapted(inputs, weight, down_a, first_up_map, indicator_rows):
    low_rank = low_back(low(product('gti,gir->gtr', inputs, product('ge,eir->gir', indicator_rows, down_a))))
    result = product('gti,io->gto', inputs, weight)
    return result + product('gtr,gro->gto', low_rank, product('ge,ero->gro', indicator_rows, first_up_map))

def feed_forward(resid, indicator_rows, params, ff_index):
    normed = low(layer_norm(resid, params['ln_gain'][3 * ff_index], params['ln_shift'][3 * ff_index]))
    hidden = low_back(adapted(normed, params['up'][ff_index], params['in_a'][5 * ff_index], params['up_b'][ff_index], indicator_rows))
    active = low(jax.nn.silu(hidden))
    branch = low_back(adapted(active, params['down'][ff_index], params['down_a'][ff_index], params['out_b'][3 * ff_index], indicator_rows))
    return resid + 0.5 * branch

def attention(resid, indicator_rows, params):
    group_size, length, width_all = resid.shape
    head_dim = width_all // HEADS
    normed = low(layer_norm(resid, params['ln_gain'][1], params['ln_shift'][1]))
    projections = []
    for part_index in range(3):
        projected = adapted(normed, params['qkv'][:, part_index], params['in_a'][1 + part_index], params['qkv_b'][part_index], indicator_rows)
        projections.append(low_back(low(projected)).reshape(group_size, length, HEADS, head_dim))
    scores = low_back(product('gqhe,gkhe->ghqk', projections[0], projections[1]))
    weights = jax.nn.softmax(scores * head_dim ** (-0.5), axis=-1)
    attended = product('ghqk,gkhe->gqhe', low(weights), projections[2])
    attended = low_back(low(attended.reshape(group_size, length, width_all)))
    branch = low_back(adapted(attended, params['attn_out'], params['mix_a'][0], params['out_b'][1], indicator_rows))
    return resid + branch

def conv_front(resid, indicator_rows, params):
    group_size, length, width_all = resid.shape
    normed = low(layer_norm(resid, params['ln_gain'][2], params['ln_shift'][2]))
    glu_table = params['glu_b']
    joined = adapted(normed, params['glu'].reshape(width_all, 2 * width_all), params['in_a'][4], glu_table.reshape(glu_table.shape[0], glu_table.shape[1], 2 * width_all), indicator_rows)
    joined = low_back(joined.reshape(group_size, length, 2, width_all))
    gated = low(joined[:, :, 0] * jax.nn.sigmoid(joined[:, :, 1]))
    kernel = params['depth']
    half_width = kernel.shape[0] // 2
    padded = jnp.pad(gated, ((0, 0), (half_width, half_width), (0, 0)))
    mixed_sum = padded[:, 0:length] * kernel[0]
    for tap_index in range(1, kernel.shape[0]):
        mixed_sum = mixed_sum + padded[:, tap_index:tap_index + length] * kernel[tap_index]
    return low_back(mixed_sum)

def encoder_layer(resid, indicator_rows, params, group_size):
    seq_total, length, width_all = resid.shape
    blocks = seq_total // group_size
    grouped = resid.reshape(blocks, group_size, length, width_all)
    grouped_hot = indicator_rows.reshape(blocks, group_size, indicator_rows.shape[-1])

    def front_half(operands):
        segment, segment_hot = operands
        segment = feed_forward(segment, segment_hot, params, 0)
        segment = attention(segment, segment_hot, params)
        return (segment, conv_front(segment, segment_hot, params))
    states, mixed_all = lax.map(jax.checkpoint(front_half), (grouped, grouped_hot))
    centre = lax.optimization_barrier(jnp.mean(mixed_all, axis=(0, 1, 2)))
    centred = mixed_all - centre
    variance = lax.optimization_barrier(jnp.mean(centred * centred, axis=(0, 1, 2)))

    def back_half(operands):
        segment, segment_mixed, segment_hot = operands
        normalized = (segment_mixed - centre) * lax.rsqrt(variance + EPS) * params['bn_gain'] + params['bn_shift']
        active = low(jax.nn.silu(normalized))
        branch = low_back(adapted(active, params['conv_out'], params['mix_a'][1], params['out_b'][2], segment_hot))
        segment = feed_forward(segment + branch, segment_hot, params, 1)
        return layer_norm(segment, params['ln_gain'][4], params['ln_shift'][4])
    result = lax.map(jax.checkpoint(back_half), (states, mixed_all, grouped_hot))
    return result.reshape(seq_total, length, width_all)

def reference(frames, sequence_adapter, feedforward_up_weight, feedforward_down_weight, query_key_value_weight, attention_output_weight, pointwise_first_weight, depthwise_weight, batchnorm_scale, batchnorm_bias, pointwise_second_weight, layernorm_scale, layernorm_bias, adapter_reader_down, adapter_first_up, adapter_query_key_up, adapter_gating_up, adapter_second_down, adapter_mixing_down, adapter_writer_up, final_output_gradient):
    indicator_rows = (sequence_adapter[:, None] == jnp.arange(ADAPTER_NUMBER, dtype=jnp.int32)[None, :]).astype(jnp.float32)
    group_size = math.gcd(SEQS, max(1, 4096 // LEN))
    up_all = feedforward_up_weight.astype(jnp.float32)
    down_all = feedforward_down_weight.astype(jnp.float32)
    qkv_all = query_key_value_weight.astype(jnp.float32)
    attn_out_all = attention_output_weight.astype(jnp.float32)
    glu_all = pointwise_first_weight.astype(jnp.float32)
    conv_out_all = pointwise_second_weight.astype(jnp.float32)

    def forward_call(inputs, reader_down_map, first_up_map, query_key_up_map, gating_up_map, down_a, mixing_down_map, writer_up_map):
        resid = inputs
        for layer_position in range(ENCODER_DEPTH):
            params = {'up': up_all[layer_position], 'down': down_all[layer_position], 'qkv': qkv_all[layer_position], 'attn_out': attn_out_all[layer_position], 'glu': glu_all[layer_position], 'conv_out': conv_out_all[layer_position], 'depth': depthwise_weight[layer_position], 'bn_gain': batchnorm_scale[layer_position], 'bn_shift': batchnorm_bias[layer_position], 'ln_gain': layernorm_scale[layer_position], 'ln_shift': layernorm_bias[layer_position], 'in_a': reader_down_map[layer_position], 'up_b': first_up_map[layer_position], 'qkv_b': query_key_up_map[layer_position], 'glu_b': gating_up_map[layer_position], 'down_a': down_a[layer_position], 'mix_a': mixing_down_map[layer_position], 'out_b': writer_up_map[layer_position]}
            resid = encoder_layer(resid, indicator_rows, params, group_size)
        return resid
    encoded, reverse_function = jax.vjp(forward_call, frames.astype(jnp.float32), adapter_reader_down.astype(jnp.float32), adapter_first_up.astype(jnp.float32), adapter_query_key_up.astype(jnp.float32), adapter_gating_up.astype(jnp.float32), adapter_second_down.astype(jnp.float32), adapter_mixing_down.astype(jnp.float32), adapter_writer_up.astype(jnp.float32))
    grads = reverse_function(final_output_gradient.astype(jnp.float32))
    return (encoded.astype(jnp.bfloat16), grads[0], grads[1], grads[2], grads[3], grads[4], grads[5], grads[6], grads[7])
```

```python
import jax
import jax.numpy as jnp
from jax import lax
from jax.sharding import PartitionSpec as P

HEADS = 8


EPS = 1e-05
NARROW = jnp.bfloat16
SINGLE = jnp.float32


def swap(value, axis, offset):
    count = lax.axis_size(axis)
    return lax.ppermute(value, axis, [(i, i ^ offset) for i in range(count)])


def offsets_of(axis):
    return range(1, lax.axis_size(axis))


def bits_of(axis):
    count = lax.axis_size(axis)
    assert count & (count - 1) == 0
    return [1 << i for i in range(count.bit_length() - 1)]


def in_order(mine, other, axis, bit):
    upper = (lax.axis_index(axis) & bit) != 0
    return (jnp.where(upper, other, mine), jnp.where(upper, mine, other))


def doubling_gather(block, axis, dim):
    for bit in bits_of(axis):
        block = jnp.concatenate(in_order(block, swap(block, axis, bit), axis, bit), axis=dim)
    return block


def two_way_gather(block, axis, dim):
    bits = bits_of(axis)
    count = lax.axis_size(axis)
    other = 1 - dim
    half = block.shape[other] // 2
    pieces = []
    for part, order in enumerate((bits, bits[::-1])):
        held = {0: lax.slice_in_dim(block, part * half, (part + 1) * half, axis=other)}
        for bit in order:
            names = sorted(held)
            sent = jnp.concatenate([held[n] for n in names], axis=dim)
            came = swap(sent, axis, bit)
            size = block.shape[dim]
            for spot, n in enumerate(names):
                got = lax.slice_in_dim(came, spot * size, (spot + 1) * size, axis=dim)
                low, high = in_order(held[n], got, axis, bit)
                held[n] = low
                held[n | bit] = high
        pieces.append(jnp.concatenate([held[n] for n in range(count)], axis=dim))
    return jnp.concatenate(pieces, axis=other)


def full_weight(shard, gather_dim):
    other = 1 - gather_dim
    part = shard.shape[other] // lax.axis_size("ctx")
    mine = lax.dynamic_slice_in_dim(shard, lax.axis_index("ctx") * part, part, other)
    return two_way_gather(doubling_gather(mine, "fsdp", gather_dim), "ctx", other)


def pair_sum(partial):
    low = partial.astype(NARROW)
    return low.astype(SINGLE) + swap(low, "tp", 1).astype(SINGLE)


def block_at(value, index, size, dim):
    return lax.dynamic_slice_in_dim(value, index * size, size, dim)


def by_owner(pieces, axis):
    me = lax.axis_index(axis)
    pieces = list(pieces)
    for bit in bits_of(axis):
        upper = (me & bit) != 0
        pieces = [jnp.where(upper, pieces[k ^ bit], pieces[k]) for k in range(len(pieces))]
    return pieces


def heads_out(value, axis):
    width = value.shape[-1] // lax.axis_size(axis)
    me = lax.axis_index(axis)
    got = [block_at(value, me, width, value.ndim - 1)]
    for k in offsets_of(axis):
        got.append(swap(block_at(value, me ^ k, width, value.ndim - 1), axis, k))
    return got


def heads_back(value, axis, dim):
    size = value.shape[dim] // lax.axis_size(axis)
    got = [lax.slice_in_dim(value, 0, size, axis=dim)]
    for k in offsets_of(axis):
        got.append(swap(lax.slice_in_dim(value, k * size, (k + 1) * size, axis=dim), axis, k))
    return by_owner(got, axis)


def with_halo(cells, sides, width):
    for axis, dim in sides:
        count = lax.axis_size(axis)
        ends = count - 1
        head = lax.slice_in_dim(cells, 0, width, axis=dim)
        tail = lax.slice_in_dim(cells, cells.shape[dim] - width, cells.shape[dim], axis=dim)
        cells = jnp.concatenate(
            [
                lax.ppermute(tail, axis, [(i, (i + 1) % count) for i in range(ends)]),
                cells,
                lax.ppermute(head, axis, [((i + 1) % count, i) for i in range(ends)]),
            ],
            axis=dim,
        )
    return cells


def layer_norm(values, gain_row, shift_row):
    centre = jnp.mean(values, axis=-1, keepdims=True)
    centred = values - centre
    spread = jnp.mean(centred * centred, axis=-1, keepdims=True)
    return centred * lax.rsqrt(spread + EPS) * gain_row + shift_row


def norm_backward(values, gain_row, shift_row, upstream):
    return jax.vjp(lambda inner_values: layer_norm(inner_values, gain_row, shift_row), values)[1](
        upstream
    )[0]


def silu_backward(values, upstream):
    return jax.vjp(jax.nn.silu, values)[1](upstream)[0]


def glu_gate(joined):
    return joined[:, :, 0] * jax.nn.sigmoid(joined[:, :, 1])


def choose_adapter(spec, indicator_rows, table):
    return jnp.einsum(spec, indicator_rows, table, preferred_element_type=SINGLE).astype(NARROW)


def adapter_sums(tables, sequence_adapter, adapter_number):
    devices = lax.axis_size("ctx")
    me = lax.axis_index("ctx")
    groups = lax.axis_size("fsdp")
    group = lax.axis_index("fsdp")
    seqs, _, rank, _ = tables[0].shape
    parts = []
    for spot in range(devices):
        pieces = []
        for table in tables:
            size = table.shape[3] // devices
            for row in range(table.shape[1]):
                pieces.append(table[:, row, :, spot * size : (spot + 1) * size])
        parts.append(jnp.concatenate(pieces, axis=2).astype(NARROW))
    spread = jnp.stack(parts)
    total = lax.dynamic_index_in_dim(spread, me, 0, False).astype(SINGLE)
    for k in offsets_of("ctx"):
        total = total + swap(
            lax.dynamic_index_in_dim(spread, me ^ k, 0, False), "ctx", k
        ).astype(SINGLE)
    share = rank // groups
    adapters = jnp.arange(adapter_number, dtype=jnp.int32)
    result = 0.0
    for k in range(groups):
        piece = block_at(total, group ^ k, share, 1)
        if k > 0:
            piece = swap(piece, "fsdp", k)
        ids = lax.dynamic_slice_in_dim(sequence_adapter, (group ^ k) * seqs, seqs)
        for row in range(seqs):
            chosen = (ids[row] == adapters)[:, None, None]
            result = result + jnp.where(chosen, piece[row][None], 0.0)
    low = result.astype(NARROW)
    pieces = by_owner([low] + [swap(low, "ctx", k) for k in offsets_of("ctx")], "ctx")
    results = []
    begin = 0
    for table in tables:
        size = table.shape[3] // devices
        rows = []
        for row in range(table.shape[1]):
            rows.append(
                jnp.concatenate([p[:, :, begin : begin + size] for p in pieces], axis=2)
            )
            begin += size
        results.append(jnp.stack(rows).astype(SINGLE))
    return results


def widen_rank(low_rank, parts_count):
    return jnp.broadcast_to(low_rank, low_rank.shape[:2] + (parts_count, low_rank.shape[3]))


def column_forward(inputs, weight, down_a, first_up_map):
    low_rank = jnp.einsum("std,skdr->stkr", inputs, down_a, preferred_element_type=SINGLE).astype(
        NARROW
    )
    result = jnp.einsum("std,djo->stjo", inputs, weight, preferred_element_type=SINGLE)
    result = result + jnp.einsum(
        "stjr,sjro->stjo",
        widen_rank(low_rank, first_up_map.shape[1]),
        first_up_map,
        preferred_element_type=SINGLE,
    )
    return (result, low_rank)


def column_backward(grad_low, inputs, low_rank, weight, down_a, first_up_map):
    grad_up = jnp.einsum(
        "stjr,stjo->sjro",
        widen_rank(low_rank, first_up_map.shape[1]),
        grad_low,
        preferred_element_type=SINGLE,
    )
    main_part = jnp.einsum("stjo,djo->std", grad_low, weight, preferred_element_type=SINGLE)
    rank_part = jnp.einsum("stjo,sjro->stjr", grad_low, first_up_map, preferred_element_type=SINGLE)
    if down_a.shape[1] != first_up_map.shape[1]:
        rank_part = jnp.sum(rank_part, axis=2, keepdims=True)
    main_part, rank_part = (pair_sum(main_part), pair_sum(rank_part))
    rank_grad = rank_part.astype(NARROW)
    grad_down = jnp.einsum("std,stkr->skrd", inputs, rank_grad, preferred_element_type=SINGLE)
    input_grad = main_part + jnp.einsum(
        "stkr,skdr->std", rank_grad, down_a, preferred_element_type=SINGLE
    )
    return (input_grad, grad_down, grad_up)


def row_forward(inputs, weight, down_a, first_up_map):
    main_part = jnp.einsum("stf,fd->std", inputs, weight, preferred_element_type=SINGLE)
    rank_part = jnp.einsum("stf,sfr->str", inputs, down_a, preferred_element_type=SINGLE)
    main_part, rank_part = (pair_sum(main_part), pair_sum(rank_part))
    low_rank = rank_part.astype(NARROW)
    return (
        main_part
        + jnp.einsum("str,srd->std", low_rank, first_up_map, preferred_element_type=SINGLE),
        low_rank,
    )


def row_backward(branch_low, inputs, low_rank, weight, down_a, first_up_map):
    rank_grad = jnp.einsum(
        "std,srd->str", branch_low, first_up_map, preferred_element_type=SINGLE
    ).astype(NARROW)
    grad_up = jnp.einsum("str,std->srd", low_rank, branch_low, preferred_element_type=SINGLE)
    grad_down = jnp.einsum("stf,str->srf", inputs, rank_grad, preferred_element_type=SINGLE)
    input_grad = jnp.einsum("std,fd->stf", branch_low, weight, preferred_element_type=SINGLE)
    input_grad = input_grad + jnp.einsum(
        "str,sfr->stf", rank_grad, down_a, preferred_element_type=SINGLE
    )
    return (input_grad, grad_down, grad_up)


def depthwise(padded, kernel, length):
    running = padded[:, 0:length].astype(SINGLE) * kernel[0]
    for tap_index in range(1, kernel.shape[0]):
        running = (
            running + padded[:, tap_index : tap_index + length].astype(SINGLE) * kernel[tap_index]
        )
    return running


def depthwise_back(padded_grad, kernel, length):
    tap_count = kernel.shape[0]
    running = padded_grad[:, tap_count - 1 : tap_count - 1 + length].astype(SINGLE) * kernel[0]
    for tap_index in range(1, tap_count):
        begin_at = tap_count - 1 - tap_index
        running = (
            running
            + padded_grad[:, begin_at : begin_at + length].astype(SINGLE) * kernel[tap_index]
        )
    return running


def split_heads(values, head_dim):
    return values.reshape(values.shape[0], values.shape[1], values.shape[2] // head_dim, head_dim)


def attention_forward(query, key_all, value_all, head_dim, score_scale):
    seq_count, query_rows, local_width = query.shape
    scores = (
        jnp.einsum(
            "sqhe,skhe->shqk",
            split_heads(query, head_dim),
            split_heads(key_all, head_dim),
            preferred_element_type=SINGLE,
        )
        * score_scale
    )
    highest = jnp.max(scores, axis=-1, keepdims=True)
    exponent = jnp.exp(scores - highest)
    row_total = jnp.sum(exponent, axis=-1, keepdims=True)
    weights_low = (exponent / row_total).astype(NARROW)
    attended = jnp.einsum(
        "shqk,skhe->sqhe",
        weights_low,
        split_heads(value_all, head_dim),
        preferred_element_type=SINGLE,
    )
    return (
        attended.reshape(seq_count, query_rows, local_width).astype(NARROW),
        highest + jnp.log(row_total),
    )


def attention_backward(query, key_all, value_all, log_total, grad_low, head_dim, score_scale):
    seq_count, query_rows, local_width = query.shape
    query_heads = split_heads(query, head_dim)
    key_heads = split_heads(key_all, head_dim)
    grad_heads = split_heads(grad_low, head_dim)
    probs = jnp.exp(
        jnp.einsum("sqhe,skhe->shqk", query_heads, key_heads, preferred_element_type=SINGLE)
        * score_scale
        - log_total
    )
    prob_grad = jnp.einsum(
        "sqhe,skhe->shqk",
        grad_heads,
        split_heads(value_all, head_dim),
        preferred_element_type=SINGLE,
    )
    value_grad = jnp.einsum(
        "shqk,sqhe->skhe", probs.astype(NARROW), grad_heads, preferred_element_type=SINGLE
    )
    row_dot = jnp.sum(probs * prob_grad, axis=-1, keepdims=True)
    score_grad = (score_scale * probs * (prob_grad - row_dot)).astype(NARROW)
    query_grad = jnp.einsum("shqk,skhe->sqhe", score_grad, key_heads, preferred_element_type=SINGLE)
    key_grad = jnp.einsum("shqk,sqhe->skhe", score_grad, query_heads, preferred_element_type=SINGLE)
    key_rows = key_all.shape[1]
    return (
        query_grad.reshape(seq_count, query_rows, local_width),
        key_grad.reshape(seq_count, key_rows, local_width),
        value_grad.reshape(seq_count, key_rows, local_width),
    )


def per_device(
    frames,
    sequence_adapter,
    feedforward_up_weight,
    feedforward_down_weight,
    query_key_value_weight,
    attention_output_weight,
    pointwise_first_weight,
    depthwise_weight,
    batchnorm_scale,
    batchnorm_bias,
    pointwise_second_weight,
    layernorm_scale,
    layernorm_bias,
    adapter_reader_down,
    adapter_first_up,
    adapter_query_key_up,
    adapter_gating_up,
    adapter_second_down,
    adapter_mixing_down,
    adapter_writer_up,
    final_output_gradient,
):
    layer_total = feedforward_up_weight.shape[0]
    seq_count, local_rows, model_width = frames.shape
    head_dim = model_width // HEADS
    score_scale = head_dim ** (-0.5)
    tensor_index = lax.axis_index("tp")
    tensor_count = lax.axis_size("tp")
    token_count = seq_count * local_rows * lax.axis_size("fsdp") * lax.axis_size("ctx")
    adapter_number = adapter_reader_down.shape[2]
    half_width = depthwise_weight.shape[1] // 2
    adapter_range = jnp.arange(adapter_number, dtype=jnp.int32)
    own_ids = lax.dynamic_slice_in_dim(
        sequence_adapter, lax.axis_index("fsdp") * seq_count, seq_count
    )
    indicator_rows = (own_ids[:, None] == adapter_range[None, :]).astype(NARROW)

    def shard_section(table, axis_index):
        part_size = table.shape[axis_index] // tensor_count
        return lax.dynamic_slice_in_dim(table, tensor_index * part_size, part_size, axis_index)

    def ff_forward(resid, weights, picked, layer_position, ff_index):
        normed = layer_norm(
            resid,
            layernorm_scale[layer_position, 3 * ff_index],
            layernorm_bias[layer_position, 3 * ff_index],
        ).astype(NARROW)
        hidden, low_in = column_forward(
            normed,
            weights["up"][ff_index][:, None, :],
            picked["in_a"][:, 5 * ff_index : 5 * ff_index + 1],
            picked["up_b"][:, ff_index : ff_index + 1],
        )
        hidden = hidden[:, :, 0]
        active = jax.nn.silu(hidden).astype(NARROW)
        branch, low_out = row_forward(
            active,
            weights["down"][ff_index],
            picked["down_a"][:, ff_index],
            picked["out_b"][:, 3 * ff_index],
        )
        return (resid + 0.5 * branch, (normed, low_in, hidden, active, low_out))

    def ff_backward(resid_grad, state, weights, picked, layer_position, ff_index, cache):
        normed, low_in, hidden, active, low_out = cache
        branch_low = (0.5 * resid_grad).astype(NARROW)
        active_grad, grad_down, grad_out = row_backward(
            branch_low,
            active,
            low_out,
            weights["down"][ff_index],
            picked["down_a"][:, ff_index],
            picked["out_b"][:, 3 * ff_index],
        )
        hidden_grad = silu_backward(hidden, active_grad).astype(NARROW)
        normed_grad, grad_in, grad_up = column_backward(
            hidden_grad[:, :, None],
            normed,
            low_in,
            weights["up"][ff_index][:, None, :],
            picked["in_a"][:, 5 * ff_index : 5 * ff_index + 1],
            picked["up_b"][:, ff_index : ff_index + 1],
        )
        resid_grad = resid_grad + norm_backward(
            state,
            layernorm_scale[layer_position, 3 * ff_index],
            layernorm_bias[layer_position, 3 * ff_index],
            normed_grad,
        )
        return (resid_grad, (grad_in, grad_up, grad_down, grad_out))

    resid = frames.astype(SINGLE)
    kept_weights = []
    layer_position = 0
    weights = {
        "up": [None, None],
        "down": [None, None],
    }
    flat_qkv = query_key_value_weight[layer_position].reshape(query_key_value_weight.shape[1], -1)
    flat_glu = pointwise_first_weight[layer_position].reshape(pointwise_first_weight.shape[1], -1)
    weights["up"][0] = full_weight(feedforward_up_weight[layer_position, 0], 0)
    weights["down"][0] = full_weight(feedforward_down_weight[layer_position, 0], 1)
    weights["qkv"] = full_weight(flat_qkv, 0).reshape((model_width,) + query_key_value_weight.shape[2:])
    weights["attn_out"] = full_weight(attention_output_weight[layer_position], 1)
    weights["glu"] = full_weight(flat_glu, 0).reshape((model_width,) + pointwise_first_weight.shape[2:])
    weights["conv_out"] = full_weight(pointwise_second_weight[layer_position], 1)
    weights["up"][1] = full_weight(feedforward_up_weight[layer_position, 1], 0)
    weights["down"][1] = full_weight(feedforward_down_weight[layer_position, 1], 1)
    picked = {
        "in_a": choose_adapter(
            "hq,iqao->hiao", indicator_rows, adapter_reader_down[layer_position]
        ),
        "up_b": choose_adapter(
            "tf,nfya->tnya", indicator_rows, shard_section(adapter_first_up[layer_position], 3)
        ),
        "qkv_b": choose_adapter(
            "tf,nfya->tnya", indicator_rows, shard_section(adapter_query_key_up[layer_position], 3)
        ),
        "glu_b": choose_adapter(
            "kq,qnfi->kfni", indicator_rows, shard_section(adapter_gating_up[layer_position], 3)
        ),
        "down_a": choose_adapter(
            "gz,fzbv->gfbv", indicator_rows, shard_section(adapter_second_down[layer_position], 2)
        ),
        "mix_a": choose_adapter(
            "gz,fzbv->gfbv", indicator_rows, shard_section(adapter_mixing_down[layer_position], 2)
        ),
        "out_b": choose_adapter("vf,tfhk->vthk", indicator_rows, adapter_writer_up[layer_position]),
    }
    states = [resid]
    resid, ff_first = ff_forward(resid, weights, picked, layer_position, 0)
    states.append(resid)
    normed = layer_norm(
        resid, layernorm_scale[layer_position, 1], layernorm_bias[layer_position, 1]
    ).astype(NARROW)
    projected, low_in = column_forward(
        normed, weights["qkv"], picked["in_a"][:, 1:4], picked["qkv_b"]
    )
    projected = projected.astype(NARROW)
    query, key_all, value_all = (
        jnp.concatenate(part, axis=1)
        for part in zip(
            *[
                (got[:, :, 0], got[:, :, 1], got[:, :, 2])
                for got in heads_out(projected, "ctx")
            ]
        )
    )
    attended_heads, log_total = attention_forward(query, key_all, value_all, head_dim, score_scale)
    attended = jnp.concatenate(heads_back(attended_heads, "ctx", 1), axis=2)
    branch, low_out = row_forward(
        attended, weights["attn_out"], picked["mix_a"][:, 0], picked["out_b"][:, 1]
    )
    resid, attn_cache = (
        resid + branch,
        (normed, low_in, query, key_all, value_all, log_total, attended, low_out),
    )
    states.append(resid)
    kernel = depthwise_weight[layer_position]
    normed = layer_norm(
        resid, layernorm_scale[layer_position, 2], layernorm_bias[layer_position, 2]
    ).astype(NARROW)
    projected, low_in = column_forward(
        normed, weights["glu"], picked["in_a"][:, 4:5], picked["glu_b"]
    )
    gated = glu_gate(projected).astype(NARROW)
    padded = with_halo(gated, (("ctx", 1),), half_width)
    mixed_sum = depthwise(padded, kernel, local_rows)
    centre = jnp.mean(mixed_sum, axis=(0, 1))
    spread = mixed_sum - centre
    spread = jnp.sum(spread * spread, axis=(0, 1))
    gathered_count = seq_count * local_rows
    for axis in ("ctx", "fsdp"):
        for bit in bits_of(axis):
            own = jnp.stack((centre, spread))
            met = swap(own, axis, bit)
            apart = centre - met[0]
            spread = spread + met[1] + apart * apart * (0.5 * gathered_count)
            centre = 0.5 * (centre + met[0])
            gathered_count = 2 * gathered_count
    centred = mixed_sum - centre
    variance = spread / token_count
    inv_std = lax.rsqrt(variance + EPS)
    standard = centred * inv_std
    normalized = standard * batchnorm_scale[layer_position] + batchnorm_bias[layer_position]
    active = jax.nn.silu(normalized).astype(NARROW)
    branch, low_out = row_forward(
        active, weights["conv_out"], picked["mix_a"][:, 1], picked["out_b"][:, 2]
    )
    resid, conv_cache = (
        resid + branch,
        (normed, low_in, projected, standard, inv_std, normalized, active, low_out),
    )
    states.append(resid)
    resid, ff_last = ff_forward(resid, weights, picked, layer_position, 1)
    states.append(resid)
    resid = layer_norm(resid, layernorm_scale[layer_position, 4], layernorm_bias[layer_position, 4])
    caches = [(states, ff_first, attn_cache, conv_cache, ff_last)]
    kept_weights.append(weights)
    selections = [picked]
    encoded = resid.astype(NARROW)
    resid_grad = final_output_gradient.astype(SINGLE)
    layer_seqs = [None] * layer_total
    for layer_position in reversed(range(layer_total)):
        weights = kept_weights[layer_position]
        picked = selections[layer_position]
        states, ff_first, attn_cache, conv_cache, ff_last = caches[layer_position]
        resid_grad = norm_backward(
            states[4],
            layernorm_scale[layer_position, 4],
            layernorm_bias[layer_position, 4],
            resid_grad,
        )
        resid_grad, last_grads = ff_backward(
            resid_grad, states[3], weights, picked, layer_position, 1, ff_last
        )
        conv_resid_grad = resid_grad
        (
            conv_normed,
            conv_low_in,
            conv_projected,
            conv_standard,
            conv_inv_std,
            conv_normalized,
            conv_active,
            conv_low_out,
        ) = conv_cache
        conv_kernel = depthwise_weight[layer_position]
        conv_branch_low = conv_resid_grad.astype(NARROW)
        conv_active_grad, grad_mix, conv_grad_out = row_backward(
            conv_branch_low,
            conv_active,
            conv_low_out,
            weights["conv_out"],
            picked["mix_a"][:, 1],
            picked["out_b"][:, 2],
        )
        standard_grad = (
            silu_backward(conv_normalized, conv_active_grad) * batchnorm_scale[layer_position]
        )
        grad_pair = jnp.stack(
            (
                jnp.sum(standard_grad, axis=(0, 1)),
                jnp.sum(standard_grad * conv_standard, axis=(0, 1)),
            )
        )
        for axis in ("ctx", "fsdp"):
            for bit in bits_of(axis):
                grad_pair = grad_pair + swap(grad_pair, axis, bit)
        grad_first, grad_second = (grad_pair[0], grad_pair[1])
        mixed_grad = (
            conv_inv_std
            * (
                standard_grad
                - grad_first / token_count
                - conv_standard * (grad_second / token_count)
            )
        ).astype(NARROW)
        padded_grad = with_halo(mixed_grad, (("ctx", 1),), half_width)
        gated_grad = depthwise_back(padded_grad, conv_kernel, local_rows)
        projected_grad = jax.vjp(glu_gate, conv_projected)[1](gated_grad)[0].astype(NARROW)
        conv_normed_grad, conv_grad_in, grad_glu = column_backward(
            projected_grad,
            conv_normed,
            conv_low_in,
            weights["glu"],
            picked["in_a"][:, 4:5],
            picked["glu_b"],
        )
        conv_resid_grad = conv_resid_grad + norm_backward(
            states[2],
            layernorm_scale[layer_position, 2],
            layernorm_bias[layer_position, 2],
            conv_normed_grad,
        )
        resid_grad = conv_resid_grad
        conv_grads = (conv_grad_in, grad_glu, grad_mix, conv_grad_out)
        attention_resid_grad = resid_grad
        (
            attention_normed,
            attention_low_in,
            attention_query,
            attention_key_all,
            attention_value_all,
            attention_log_total,
            attention_attended,
            attention_low_out,
        ) = attn_cache
        attention_branch_low = attention_resid_grad.astype(NARROW)
        attended_grad, attention_grad_mix, attention_grad_out = row_backward(
            attention_branch_low,
            attention_attended,
            attention_low_out,
            weights["attn_out"],
            picked["mix_a"][:, 0],
            picked["out_b"][:, 1],
        )
        attended_grad_heads = jnp.concatenate(
            heads_out(attended_grad.astype(NARROW), "ctx"), axis=1
        )
        head_grads = attention_backward(
            attention_query,
            attention_key_all,
            attention_value_all,
            attention_log_total,
            attended_grad_heads,
            head_dim,
            score_scale,
        )
        attention_projected_grad = jnp.concatenate(
            heads_back(jnp.stack(head_grads, axis=2).astype(NARROW), "ctx", 1), axis=3
        )
        attention_normed_grad, attention_grad_in, grad_qkv = column_backward(
            attention_projected_grad,
            attention_normed,
            attention_low_in,
            weights["qkv"],
            picked["in_a"][:, 1:4],
            picked["qkv_b"],
        )
        attention_resid_grad = attention_resid_grad + norm_backward(
            states[1],
            layernorm_scale[layer_position, 1],
            layernorm_bias[layer_position, 1],
            attention_normed_grad,
        )
        resid_grad = attention_resid_grad
        attn_grads = (attention_grad_in, grad_qkv, attention_grad_mix, attention_grad_out)
        resid_grad, first_grads = ff_backward(
            resid_grad, states[0], weights, picked, layer_position, 0, ff_first
        )
        layer_seqs[layer_position] = (
            jnp.concatenate((first_grads[0], attn_grads[0], conv_grads[0], last_grads[0]), axis=1),
            jnp.concatenate((first_grads[1], last_grads[1]), axis=1),
            attn_grads[1],
            conv_grads[1],
            jnp.stack((first_grads[2], last_grads[2]), axis=1),
            jnp.stack((attn_grads[2], conv_grads[2]), axis=1),
            jnp.stack((first_grads[3], attn_grads[3], conv_grads[3], last_grads[3]), axis=1),
        )
    totals = adapter_sums(layer_seqs[0], sequence_adapter, adapter_number)
    totals = (
        jnp.swapaxes(totals[0], 2, 3)[None],
        totals[1][None],
        totals[2][None],
        jnp.transpose(totals[3], (1, 2, 0, 3))[None],
        jnp.swapaxes(totals[4], 2, 3)[None],
        jnp.swapaxes(totals[5], 2, 3)[None],
        totals[6][None],
    )
    return (
        encoded,
        resid_grad,
        totals[0],
        totals[1],
        totals[2],
        totals[3],
        totals[4],
        totals[5],
        totals[6],
    )


def solution(mesh):
    placed = (
        P("fsdp", "ctx", None),
        P(),
        P(None, None, "fsdp", "tp"),
        P(None, None, "tp", "fsdp"),
        P(None, "fsdp", None, "tp"),
        P(None, "tp", "fsdp"),
        P(None, "fsdp", None, "tp"),
        P(None, None, "tp"),
        P(None, "tp"),
        P(None, "tp"),
        P(None, "tp", "fsdp"),
        P(),
        P(),
        P(),
        P(),
        P(),
        P(),
        P(),
        P(),
        P(),
        P("fsdp", "ctx", None),
    )
    return jax.shard_map(
        per_device,
        mesh=mesh,
        in_specs=placed,
        out_specs=(
            P("fsdp", "ctx", None),
            P("fsdp", "ctx", None),
            P(None, None, None, None, "fsdp"),
            P(None, None, None, "fsdp", "tp"),
            P(None, None, None, "fsdp", "tp"),
            P(None, None, "fsdp", None, "tp"),
            P(None, None, None, "tp", "fsdp"),
            P(None, None, None, "tp", "fsdp"),
            P(None, None, None, "fsdp", None),
        ),
        check_vma=False,
    )
```

```python
import jax
import jax.numpy as jnp
from jax import lax
from jax.sharding import PartitionSpec as P

HEADS = 8


EPS = 1e-05
NARROW = jnp.bfloat16
SINGLE = jnp.float32


def swap(value, axis, offset):
    count = lax.axis_size(axis)
    return lax.ppermute(value, axis, [(i, i ^ offset) for i in range(count)])


def offsets_of(axis):
    return range(1, lax.axis_size(axis))


def bits_of(axis):
    count = lax.axis_size(axis)
    assert count & (count - 1) == 0
    return [1 << i for i in range(count.bit_length() - 1)]


def settled(value):
    return lax.optimization_barrier(value)


def in_order(mine, other, axis, bit):
    upper = (lax.axis_index(axis) & bit) != 0
    return (jnp.where(upper, other, mine), jnp.where(upper, mine, other))


def by_owner(pieces, axis):
    me = lax.axis_index(axis)
    pieces = list(pieces)
    for bit in bits_of(axis):
        upper = (me & bit) != 0
        pieces = [jnp.where(upper, pieces[k ^ bit], pieces[k]) for k in range(len(pieces))]
    return pieces


def block_at(value, index, size, dim):
    return lax.dynamic_slice_in_dim(value, index * size, size, dim)


def relative_blocks(value, axis, dim):
    size = value.shape[dim] // lax.axis_size(axis)
    me = lax.axis_index(axis)
    return [block_at(value, me ^ k, size, dim) for k in range(lax.axis_size(axis))]


def weight_blocks(shard, gather_dim, low_first):
    block = shard
    for bit in bits_of("fsdp"):
        low, high = settled(in_order(block, swap(block, "fsdp", bit), "fsdp", bit))
        block = jnp.concatenate((low, high), axis=gather_dim)
    block = settled(block)
    held = {0: block}
    bits = bits_of("ctx")
    for bit in bits if low_first else bits[::-1]:
        for place in sorted(held):
            held[place ^ bit] = swap(held[place], "ctx", bit)
    return [held[place] for place in range(lax.axis_size("ctx"))]


def pair_sum(partial):
    low = partial.astype(NARROW)
    return low.astype(SINGLE) + swap(low, "tp", 1).astype(SINGLE)


def with_halo(cells, axis, dim, width):
    count = lax.axis_size(axis)
    ends = count - 1
    head = lax.slice_in_dim(cells, 0, width, axis=dim)
    tail = lax.slice_in_dim(cells, cells.shape[dim] - width, cells.shape[dim], axis=dim)
    return jnp.concatenate(
        [
            lax.ppermute(tail, axis, [(i, (i + 1) % count) for i in range(ends)]),
            cells,
            lax.ppermute(head, axis, [((i + 1) % count, i) for i in range(ends)]),
        ],
        axis=dim,
    )


def layer_norm(values, gain_row, shift_row):
    centre = jnp.mean(values, axis=-1, keepdims=True)
    centred = values - centre
    spread = jnp.mean(centred * centred, axis=-1, keepdims=True)
    return centred * lax.rsqrt(spread + EPS) * gain_row + shift_row


def norm_backward(values, gain_row, shift_row, upstream):
    return jax.vjp(lambda inner_values: layer_norm(inner_values, gain_row, shift_row), values)[1](
        upstream
    )[0]


def silu_backward(values, upstream):
    return jax.vjp(jax.nn.silu, values)[1](upstream)[0]


def glu_gate(joined):
    width = joined.shape[-1] // 2
    return joined[..., :width] * jax.nn.sigmoid(joined[..., width:])


def times(left, right):
    return jnp.einsum("ab,bc->ac", left, right, preferred_element_type=SINGLE)


def times_turned(left, right):
    return jnp.einsum("ab,cb->ac", left, right, preferred_element_type=SINGLE)


def turned_times(left, right):
    return jnp.einsum("ab,ac->bc", left, right, preferred_element_type=SINGLE)


def column_forward(inputs, joined_weight, down_rows, mask):
    low_rank = times_turned(inputs, down_rows).astype(NARROW) * mask
    joined = settled(jnp.concatenate((inputs, low_rank), axis=1))
    return (times(joined, joined_weight), joined)


def column_backward(grad_low, joined, joined_weight, down_rows, mask):
    width = down_rows.shape[1]
    grad_up = turned_times(joined[:, width:], grad_low)
    total = pair_sum(times_turned(grad_low, joined_weight))
    rank_grad = total[:, width:].astype(NARROW) * mask
    grad_down = turned_times(rank_grad, joined[:, :width])
    input_grad = total[:, :width] + times(rank_grad, down_rows)
    return (input_grad, grad_down, grad_up)


def row_forward(inputs, joined_weight, up_rows, mask):
    width = up_rows.shape[1]
    total = pair_sum(times(inputs, joined_weight))
    low_rank = total[:, width:].astype(NARROW) * mask
    return (total[:, :width] + times(low_rank, up_rows), low_rank)


def row_backward(branch_low, inputs, low_rank, joined_weight, up_rows, mask):
    rank_grad = times_turned(branch_low, up_rows).astype(NARROW) * mask
    grad_up = turned_times(low_rank, branch_low)
    grad_down = turned_times(rank_grad, inputs)
    joined = settled(jnp.concatenate((branch_low, rank_grad), axis=1))
    return (times_turned(joined, joined_weight), grad_down, grad_up)


def depthwise(padded, kernel, length):
    running = padded[:, 0:length].astype(SINGLE) * kernel[0]
    for tap_index in range(1, kernel.shape[0]):
        running = (
            running + padded[:, tap_index : tap_index + length].astype(SINGLE) * kernel[tap_index]
        )
    return running


def depthwise_back(padded_grad, kernel, length):
    tap_count = kernel.shape[0]
    running = padded_grad[:, tap_count - 1 : tap_count - 1 + length].astype(SINGLE) * kernel[0]
    for tap_index in range(1, tap_count):
        begin_at = tap_count - 1 - tap_index
        running = (
            running
            + padded_grad[:, begin_at : begin_at + length].astype(SINGLE) * kernel[tap_index]
        )
    return running


def split_heads(values, head_dim):
    return values.reshape(values.shape[0], values.shape[1], values.shape[2] // head_dim, head_dim)


def attention_forward(query, key_all, value_all, head_dim, score_scale):
    seq_count, query_rows, local_width = query.shape
    scores = (
        jnp.einsum(
            "sqhe,skhe->shqk",
            split_heads(query, head_dim),
            split_heads(key_all, head_dim),
            preferred_element_type=SINGLE,
        )
        * score_scale
    )
    highest = jnp.max(scores, axis=-1, keepdims=True)
    exponent = jnp.exp(scores - highest)
    row_total = jnp.sum(exponent, axis=-1, keepdims=True)
    weights_low = (exponent / row_total).astype(NARROW)
    attended = jnp.einsum(
        "shqk,skhe->sqhe",
        weights_low,
        split_heads(value_all, head_dim),
        preferred_element_type=SINGLE,
    )
    return (
        attended.reshape(seq_count, query_rows, local_width).astype(NARROW),
        highest + jnp.log(row_total),
    )


def attention_backward(query, key_all, value_all, log_total, grad_low, head_dim, score_scale):
    seq_count, query_rows, local_width = query.shape
    query_heads = split_heads(query, head_dim)
    key_heads = split_heads(key_all, head_dim)
    grad_heads = split_heads(grad_low, head_dim)
    probs = jnp.exp(
        jnp.einsum("sqhe,skhe->shqk", query_heads, key_heads, preferred_element_type=SINGLE)
        * score_scale
        - log_total
    )
    prob_grad = jnp.einsum(
        "sqhe,skhe->shqk",
        grad_heads,
        split_heads(value_all, head_dim),
        preferred_element_type=SINGLE,
    )
    value_grad = jnp.einsum(
        "shqk,sqhe->skhe", probs.astype(NARROW), grad_heads, preferred_element_type=SINGLE
    )
    row_dot = jnp.sum(probs * prob_grad, axis=-1, keepdims=True)
    score_grad = (score_scale * probs * (prob_grad - row_dot)).astype(NARROW)
    query_grad = jnp.einsum("shqk,skhe->sqhe", score_grad, key_heads, preferred_element_type=SINGLE)
    key_grad = jnp.einsum("shqk,sqhe->skhe", score_grad, query_heads, preferred_element_type=SINGLE)
    key_rows = key_all.shape[1]
    return (
        query_grad.reshape(seq_count, query_rows, local_width),
        key_grad.reshape(seq_count, key_rows, local_width),
        value_grad.reshape(seq_count, key_rows, local_width),
    )


def spread_rows(value, seq_count):
    count = lax.axis_size("ctx")
    width = value.shape[1] // count
    rows = value.shape[0] // seq_count
    got = []
    for k in range(count):
        piece = value[:, k * width : (k + 1) * width]
        piece = swap(settled(piece), "ctx", k) if k > 0 else piece
        got.append(piece.reshape(seq_count, rows, width))
    return settled(jnp.concatenate(got, axis=1))


def spread_columns(value):
    count = lax.axis_size("ctx")
    seq_count, rows, width = value.shape
    rows = rows // count
    got = []
    for k in range(count):
        piece = value[:, k * rows : (k + 1) * rows].reshape(seq_count * rows, width)
        got.append(swap(settled(piece), "ctx", k) if k > 0 else piece)
    return settled(jnp.concatenate(settled(got), axis=1))


def scatter_sum(tables):
    count = lax.axis_size("ctx")
    me = lax.axis_index("ctx")
    total = 0.0
    for k in range(count):
        pieces = []
        for table, relative in tables:
            size = table.shape[1] // count
            pieces.append(
                table[:, k * size : (k + 1) * size] if relative else block_at(table, me ^ k, size, 1)
            )
        joined = jnp.concatenate(settled([p.astype(NARROW) for p in pieces]), axis=1)
        if k > 0:
            joined = swap(settled(joined), "ctx", k)
        total = total + joined.astype(SINGLE)
    return total


def adapter_totals(total, sequence_adapter, adapter_number, seqs):
    groups = lax.axis_size("fsdp")
    group = lax.axis_index("fsdp")
    total = total.reshape(seqs, total.shape[0] // seqs, total.shape[1])
    share = total.shape[1] // groups
    adapters = jnp.arange(adapter_number, dtype=jnp.int32)
    result = 0.0
    for k in range(groups):
        piece = block_at(total, group ^ k, share, 1)
        if k > 0:
            piece = swap(piece, "fsdp", k)
        ids = lax.dynamic_slice_in_dim(sequence_adapter, (group ^ k) * seqs, seqs)
        for row in range(seqs):
            chosen = (ids[row] == adapters)[:, None, None]
            result = result + jnp.where(chosen, piece[row][None], 0.0)
    low = settled(result.astype(NARROW))
    return settled(by_owner([low] + [swap(low, "ctx", k) for k in offsets_of("ctx")], "ctx"))


def per_device(
    frames,
    sequence_adapter,
    feedforward_up_weight,
    feedforward_down_weight,
    query_key_value_weight,
    attention_output_weight,
    pointwise_first_weight,
    depthwise_weight,
    batchnorm_scale,
    batchnorm_bias,
    pointwise_second_weight,
    layernorm_scale,
    layernorm_bias,
    adapter_reader_down,
    adapter_first_up,
    adapter_query_key_up,
    adapter_gating_up,
    adapter_second_down,
    adapter_mixing_down,
    adapter_writer_up,
    final_output_gradient,
):
    assert feedforward_up_weight.shape[0] == 1
    seq_count, local_rows, model_width = frames.shape
    tokens = seq_count * local_rows
    head_dim = model_width // HEADS
    score_scale = head_dim ** (-0.5)
    tensor_index = lax.axis_index("tp")
    tensor_count = lax.axis_size("tp")
    ctx_index = lax.axis_index("ctx")
    ctx_count = lax.axis_size("ctx")
    token_count = tokens * lax.axis_size("fsdp") * ctx_count
    adapter_number, rank = (adapter_reader_down.shape[2], adapter_reader_down.shape[4])
    ranks = seq_count * rank
    half_width = depthwise_weight.shape[1] // 2
    own_ids = lax.dynamic_slice_in_dim(
        sequence_adapter, lax.axis_index("fsdp") * seq_count, seq_count
    )
    indicator = (
        own_ids[:, None] == jnp.arange(adapter_number, dtype=jnp.int32)[None, :]
    ).astype(NARROW)
    mask = (
        jnp.arange(tokens)[:, None] // local_rows == jnp.arange(ranks)[None, :] // rank
    ).astype(NARROW)
    mask_three = jnp.tile(mask, (1, 3))

    def chosen(spec, table):
        picked = jnp.einsum(spec, indicator, table, preferred_element_type=SINGLE).astype(NARROW)
        return picked.reshape(picked.shape[0], ranks, picked.shape[-1])

    def own_units(table, axis_index):
        size = table.shape[axis_index] // tensor_count
        return lax.dynamic_slice_in_dim(table, tensor_index * size, size, axis_index)

    def relative(table):
        return jnp.concatenate(settled(relative_blocks(table, "ctx", 2)), axis=2)

    def ctx_part(shard, dim):
        return block_at(shard, ctx_index, shard.shape[dim] // ctx_count, dim)

    in_a = chosen("sq,iqdr->isrd", adapter_reader_down[0])
    up_b = relative(chosen("sq,iqrf->isrf", own_units(adapter_first_up[0], 3)))
    qkv_b = relative(chosen("sq,iqrf->isrf", own_units(adapter_query_key_up[0], 3)))
    glu_b = chosen("sq,qrif->isrf", own_units(adapter_gating_up[0], 3))
    down_a = relative(chosen("sq,iqfr->isrf", own_units(adapter_second_down[0], 2)))
    mix_a = chosen("sq,iqfr->isrf", own_units(adapter_mixing_down[0], 2))
    out_b = chosen("sq,iqrd->isrd", adapter_writer_up[0])

    def over(blocks, rows):
        return settled(jnp.concatenate((jnp.concatenate(blocks, axis=1), rows), axis=0))

    def beside(blocks, rows):
        return settled(
            jnp.concatenate((jnp.concatenate(blocks, axis=0), settled(jnp.transpose(rows))), axis=1)
        )

    def up_weight(index):
        part = ctx_part(feedforward_up_weight[0, index], 1)
        return over(weight_blocks(part, 0, True), up_b[index])

    def down_weight(index):
        part = ctx_part(feedforward_down_weight[0, index], 0)
        return beside(weight_blocks(part, 1, False), down_a[index])

    weights = {}
    weights["up", 0] = up_weight(0)
    weights["down", 0] = down_weight(0)
    qkv_part = ctx_part(query_key_value_weight[0], 2)
    heads_width = qkv_part.shape[2]
    qkv_rows = []
    for index in range(3):
        own = qkv_b[index].reshape(ranks, ctx_count, heads_width)
        none = jnp.zeros_like(own)
        qkv_rows.append(
            jnp.stack([own if place == index else none for place in range(3)], axis=2).reshape(
                ranks, ctx_count * 3 * heads_width
            )
        )
    weights["qkv"] = over(
        weight_blocks(qkv_part.reshape(qkv_part.shape[0], -1), 0, True),
        jnp.concatenate(qkv_rows, axis=0),
    )
    weights["attn_out"] = beside(
        weight_blocks(ctx_part(attention_output_weight[0], 0), 1, False),
        relative(mix_a[0:1])[0],
    )
    glu_part = ctx_part(pointwise_first_weight[0], 2)
    glu_width = glu_part.shape[2]
    glu_blocks = settled(
        by_owner(weight_blocks(glu_part.reshape(glu_part.shape[0], -1), 0, False), "ctx")
    )
    weights["glu"] = over(
        [b[:, h * glu_width : (h + 1) * glu_width] for h in range(2) for b in glu_blocks],
        jnp.concatenate((glu_b[0], glu_b[1]), axis=1),
    )
    weights["conv_out"] = beside(
        settled(by_owner(weight_blocks(ctx_part(pointwise_second_weight[0], 0), 1, True), "ctx")),
        mix_a[1],
    )
    weights["up", 1] = up_weight(1)
    weights["down", 1] = down_weight(1)

    def normed_of(resid, index):
        return layer_norm(resid, layernorm_scale[0, index], layernorm_bias[0, index])

    def normed_back(resid, index, upstream):
        return norm_backward(resid, layernorm_scale[0, index], layernorm_bias[0, index], upstream)

    def ff_forward(resid, index):
        hidden, joined = column_forward(
            normed_of(resid, 3 * index).astype(NARROW),
            weights["up", index],
            in_a[5 * index],
            mask,
        )
        active = jax.nn.silu(hidden).astype(NARROW)
        branch, low_out = row_forward(active, weights["down", index], out_b[3 * index], mask)
        return (resid + 0.5 * branch, (joined, hidden, active, low_out))

    def ff_backward(resid_grad, state, index, cache):
        joined, hidden, active, low_out = cache
        branch_low = (0.5 * resid_grad).astype(NARROW)
        active_grad, grad_down, grad_out = row_backward(
            branch_low, active, low_out, weights["down", index], out_b[3 * index], mask
        )
        hidden_grad = settled(silu_backward(hidden, active_grad).astype(NARROW))
        normed_grad, grad_in, grad_up = column_backward(
            hidden_grad, joined, weights["up", index], in_a[5 * index], mask
        )
        resid_grad = resid_grad + normed_back(state, 3 * index, normed_grad)
        return (resid_grad, grad_in, grad_up, grad_down, grad_out)

    state_first = frames.reshape(tokens, model_width).astype(SINGLE)
    state_attn, ff_first = ff_forward(state_first, 0)

    projected, qkv_joined = column_forward(
        normed_of(state_attn, 1).astype(NARROW),
        weights["qkv"],
        in_a[1:4].reshape(3 * ranks, model_width),
        mask_three,
    )
    qkv_heads = spread_rows(settled(projected.astype(NARROW)), seq_count)
    query, key_all, value_all = (
        qkv_heads[:, :, index * heads_width : (index + 1) * heads_width] for index in range(3)
    )
    attended_heads, log_total = attention_forward(query, key_all, value_all, head_dim, score_scale)
    attended = spread_columns(settled(attended_heads))
    branch, attn_low_out = row_forward(attended, weights["attn_out"], out_b[1], mask)
    state_conv = state_attn + branch

    kernel = depthwise_weight[0]
    glu_projected, glu_joined = column_forward(
        normed_of(state_conv, 2).astype(NARROW), weights["glu"], in_a[4], mask
    )
    gated = settled(glu_gate(glu_projected).astype(NARROW)).reshape(seq_count, local_rows, -1)
    mixed_sum = depthwise(with_halo(gated, "ctx", 1, half_width), kernel, local_rows)
    centre = jnp.mean(mixed_sum, axis=(0, 1))
    spread = mixed_sum - centre
    spread = jnp.sum(spread * spread, axis=(0, 1))
    gathered_count = tokens
    for axis in ("ctx", "fsdp"):
        for bit in bits_of(axis):
            met = swap(jnp.stack((centre, spread)), axis, bit)
            apart = centre - met[0]
            spread = spread + met[1] + apart * apart * (0.5 * gathered_count)
            centre = 0.5 * (centre + met[0])
            gathered_count = 2 * gathered_count
    inv_std = lax.rsqrt(spread / token_count + EPS)
    standard = (mixed_sum - centre) * inv_std
    normalized = standard * batchnorm_scale[0] + batchnorm_bias[0]
    conv_active = jax.nn.silu(normalized).astype(NARROW).reshape(tokens, -1)
    branch, conv_low_out = row_forward(conv_active, weights["conv_out"], out_b[2], mask)
    state_last = state_conv + branch

    state_final, ff_last = ff_forward(state_last, 1)
    encoded = normed_of(state_final, 4).astype(NARROW)

    resid_grad = normed_back(
        state_final, 4, final_output_gradient.reshape(tokens, model_width).astype(SINGLE)
    )
    resid_grad, last_in, last_up, last_down, last_out = ff_backward(
        resid_grad, state_last, 1, ff_last
    )

    active_grad, conv_grad_mix, conv_grad_out = row_backward(
        resid_grad.astype(NARROW), conv_active, conv_low_out, weights["conv_out"], out_b[2], mask
    )
    standard_grad = (
        silu_backward(normalized, active_grad.reshape(normalized.shape)) * batchnorm_scale[0]
    )
    grad_pair = jnp.stack(
        (
            jnp.sum(standard_grad, axis=(0, 1)),
            jnp.sum(standard_grad * standard, axis=(0, 1)),
        )
    )
    for axis in ("ctx", "fsdp"):
        for bit in bits_of(axis):
            grad_pair = grad_pair + swap(grad_pair, axis, bit)
    mixed_grad = (
        inv_std
        * (standard_grad - grad_pair[0] / token_count - standard * (grad_pair[1] / token_count))
    ).astype(NARROW)
    gated_grad = depthwise_back(with_halo(mixed_grad, "ctx", 1, half_width), kernel, local_rows)
    projected_grad = jax.vjp(glu_gate, glu_projected)[1](gated_grad.reshape(tokens, -1))[0]
    normed_grad, conv_grad_in, grad_glu = column_backward(
        settled(projected_grad.astype(NARROW)), glu_joined, weights["glu"], in_a[4], mask
    )
    resid_grad = resid_grad + normed_back(state_conv, 2, normed_grad)
    channels = grad_glu.shape[1] // 2
    sums_last = scatter_sum(
        (
            (last_in, False),
            (conv_grad_in, False),
            (last_up, True),
            (grad_glu[:, :channels], False),
            (grad_glu[:, channels:], False),
            (last_down, True),
            (conv_grad_mix, False),
            (conv_grad_out, False),
            (last_out, False),
        )
    )

    attended_grad, attn_grad_mix, attn_grad_out = row_backward(
        resid_grad.astype(NARROW), attended, attn_low_out, weights["attn_out"], out_b[1], mask
    )
    head_grads = attention_backward(
        query,
        key_all,
        value_all,
        log_total,
        spread_rows(settled(attended_grad.astype(NARROW)), seq_count),
        head_dim,
        score_scale,
    )
    projected_grad = spread_columns(
        jnp.concatenate(settled([g.astype(NARROW) for g in head_grads]), axis=2)
    )
    normed_grad, attn_grad_in, grad_qkv = column_backward(
        projected_grad,
        qkv_joined,
        weights["qkv"],
        in_a[1:4].reshape(3 * ranks, model_width),
        mask_three,
    )
    resid_grad = resid_grad + normed_back(state_attn, 1, normed_grad)
    attn_tables = [(attn_grad_in[m * ranks : (m + 1) * ranks], False) for m in range(3)]
    for m in range(3):
        blocks = grad_qkv[m * ranks : (m + 1) * ranks]
        blocks = blocks.reshape(ranks, ctx_count, 3, heads_width)[:, :, m]
        attn_tables.append((blocks.reshape(ranks, ctx_count * heads_width), True))
    attn_tables += [(attn_grad_mix, True), (attn_grad_out, False)]
    sums_attn = scatter_sum(attn_tables)

    resid_grad, first_in, first_up, first_down, first_out = ff_backward(
        resid_grad, state_first, 0, ff_first
    )
    sums_first = scatter_sum(
        ((first_in, False), (first_up, True), (first_down, True), (first_out, False))
    )
    total = jnp.concatenate(settled((sums_last, sums_attn, sums_first)), axis=1)
    pieces = adapter_totals(total, sequence_adapter, adapter_number, seq_count)
    lengths = {
        "in": model_width,
        "up": first_up.shape[1],
        "qkv": ctx_count * heads_width,
        "glu": channels,
        "mix": conv_grad_mix.shape[1],
        "out": model_width,
    }
    lengths["down"] = lengths["up"]
    names = [
        ("in", 5), ("in", 4), ("up", 1), ("glu", 0), ("glu", 1), ("down", 1), ("mix", 1), ("out", 2), ("out", 3),
        ("in", 1), ("in", 2), ("in", 3), ("qkv", 0), ("qkv", 1), ("qkv", 2), ("mix", 0), ("out", 1),
        ("in", 0), ("up", 0), ("down", 0), ("out", 0),
    ]
    found = {}
    begin = 0
    for kind, index in names:
        size = lengths[kind] // ctx_count
        found[kind, index] = jnp.concatenate(
            [p[:, :, begin : begin + size] for p in pieces], axis=2
        ).astype(SINGLE)
        begin += size

    def table(kind):
        count = sum(1 for name, _ in names if name == kind)
        return jnp.stack([found[kind, index] for index in range(count)])

    shape = frames.shape
    return (
        encoded.reshape(shape),
        resid_grad.reshape(shape),
        jnp.swapaxes(table("in"), 2, 3)[None],
        table("up")[None],
        table("qkv")[None],
        jnp.transpose(table("glu"), (1, 2, 0, 3))[None],
        jnp.swapaxes(table("down"), 2, 3)[None],
        jnp.swapaxes(table("mix"), 2, 3)[None],
        table("out")[None],
    )


def solution(mesh):
    placed = (
        P("fsdp", "ctx", None),
        P(),
        P(None, None, "fsdp", "tp"),
        P(None, None, "tp", "fsdp"),
        P(None, "fsdp", None, "tp"),
        P(None, "tp", "fsdp"),
        P(None, "fsdp", None, "tp"),
        P(None, None, "tp"),
        P(None, "tp"),
        P(None, "tp"),
        P(None, "tp", "fsdp"),
        P(),
        P(),
        P(),
        P(),
        P(),
        P(),
        P(),
        P(),
        P(),
        P("fsdp", "ctx", None),
    )
    return jax.shard_map(
        per_device,
        mesh=mesh,
        in_specs=placed,
        out_specs=(
            P("fsdp", "ctx", None),
            P("fsdp", "ctx", None),
            P(None, None, None, None, "fsdp"),
            P(None, None, None, "fsdp", "tp"),
            P(None, None, None, "fsdp", "tp"),
            P(None, None, "fsdp", None, "tp"),
            P(None, None, None, "tp", "fsdp"),
            P(None, None, None, "tp", "fsdp"),
            P(None, None, None, "fsdp", None),
        ),
        check_vma=False,
    )
```
